32 devices in a mesh: rep: 1, dp: 32 (over x, y, z, core).
Axes of the slice: x: 2, y: 2, z: 4, core: 2. Of those that a mesh axis runs over, the one named last changes fastest.
Arguments:
- x: bfloat16 [32, 2048, 1024], P(('rep', 'dp'))
- dy: bfloat16 [32, 2048, 1024], P(('rep', 'dp'))
- w_gate: bfloat16 [2, 1024, 2816], replicated
- w_up: bfloat16 [2, 1024, 2816], replicated
- w_down: bfloat16 [2, 2816, 1024], replicated
- m_w_gate: float32 [2, 1024, 2816], P(None, 'dp')
- m_w_up: float32 [2, 1024, 2816], P(None, 'dp')
- m_w_down: float32 [2, 2816, 1024], P(None, 'dp')
- v_w_gate: float32 [2, 1024, 2816], P(None, 'dp')
- v_w_up: float32 [2, 1024, 2816], P(None, 'dp')
- v_w_down: float32 [2, 2816, 1024], P(None, 'dp')
Outputs:
- output 1: bfloat16 [2, 1024, 2816], P('rep')
- output 2: bfloat16 [2, 1024, 2816], P('rep')
- output 3: bfloat16 [2, 2816, 1024], P('rep')
- output 4: float32 [2, 1024, 2816], P('rep', 'dp')
- output 5: float32 [2, 1024, 2816], P('rep', 'dp')
- output 6: float32 [2, 2816, 1024], P('rep', 'dp')
- output 7: float32 [2, 1024, 2816], P('rep', 'dp')
- output 8: float32 [2, 1024, 2816], P('rep', 'dp')
- output 9: float32 [2, 2816, 1024], P('rep', 'dp')
All inputs are finite; a program needn't handle non-finite values.
Results may differ from the reference program's by a relative error of at most 0.02.
Values are sent between devices in bfloat16 or wider.
A program may use at most 2 GiB of HBM per device.

```python
import jax
import jax.numpy as jnp
from jax import lax

SEQUENCES = 32
TOKENS = 2048
D = 1024
FF = 2816
LAYERS = 2
NAMES = ("w_gate", "w_up", "w_down")
SHAPES = {"w_gate": (LAYERS, D, FF), "w_up": (LAYERS, D, FF), "w_down": (LAYERS, FF, D)}


def bump(key, n, height):
    away = (jnp.arange(n, dtype=jnp.int32) - jax.random.randint(key, (), 0, n, jnp.int32)) % n
    return jnp.where(away < n // 8, height, 1.0)


def together(key, own, strength):
    shared = jax.random.normal(key, own.shape[1:], jnp.float32)
    return (own + strength * shared) * lax.rsqrt(1 + strength * strength)


def setup_inputs(seed: int = 0, part: int = 0) -> dict:
    kx, kdy, ka, kb, kz, kf, kh, kl, *keys = jax.random.split(jax.random.key(seed), 8 + 3 * len(NAMES))
    kx, kdy, ka, kb = (jax.random.fold_in(k, part) for k in (kx, kdy, ka, kb))
    kw, km, kv = (keys[i::3] for i in range(3))
    shape = (SEQUENCES, TOKENS, D)
    much_x, much_dy = jax.random.uniform(kz, (2,), jnp.float32, 0.0, 1.0)
    loud = 2.0 ** jax.random.uniform(jax.random.fold_in(kz, 1), (), jnp.float32, -1.0, 2.0)
    layers = 2.0 ** jax.random.uniform(kl, (LAYERS, 1, 1), jnp.float32, -1.0, 1.0)
    x = together(ka, jax.random.normal(kx, shape, jnp.float32), much_x) * bump(kf, D, 4.0)
    dy = together(kb, jax.random.normal(kdy, shape, jnp.float32), much_dy)
    drawn = {"x": x.astype(jnp.bfloat16), "dy": (loud * dy * (SEQUENCES * TOKENS) ** -0.5).astype(jnp.bfloat16)}
    for key, name in zip(kw, NAMES, strict=True):
        w = jax.random.normal(key, SHAPES[name], jnp.float32) * SHAPES[name][1] ** -0.5
        drawn[name] = (w * {"w_gate": 1.0, "w_up": bump(kh, FF, 4.0), "w_down": layers}[name]).astype(jnp.bfloat16)
    for key, name in zip(km, NAMES, strict=True):
        drawn[f"m_{name}"] = 0.1 * jax.random.normal(key, SHAPES[name], jnp.float32)
    for key, name in zip(kv, NAMES, strict=True):
        drawn[f"v_{name}"] = jax.random.uniform(key, SHAPES[name], jnp.float32, 0.005, 0.015)
    return drawn


def matmul(a, w):
    return jnp.dot(a, w, preferred_element_type=jnp.float32).astype(jnp.bfloat16)


def normed(h):
    wide = h.astype(jnp.float32)
    scale = lax.rsqrt(jnp.mean(wide**2, -1, keepdims=True) + 1e-6)
    return (wide * scale).astype(jnp.bfloat16)


def layer(h, w):
    a = normed(h)
    gate = jnp.dot(a, w["w_gate"], preferred_element_type=jnp.float32)
    up = jnp.dot(a, w["w_up"], preferred_element_type=jnp.float32)
    return h + matmul((jax.nn.silu(gate) * up).astype(jnp.bfloat16), w["w_down"])


def adamw(w, m, v, g):
    m = 0.9 * m + 0.1 * g
    v = 0.95 * v + 0.05 * g * g
    step = m * lax.rsqrt(v + 1e-8) + 0.1 * w
    return (w - 0.02 * step).astype(jnp.bfloat16), m, v


def stack(weights, h):
    return lax.scan(lambda h, w: (layer(h, w), None), h, weights)[0]


def reference(x, dy, w_gate, w_up, w_down, m_w_gate, m_w_up, m_w_down, v_w_gate, v_w_up, v_w_down):
    weights = dict(zip(NAMES, (w_gate, w_up, w_down), strict=True))

    def take(so_far, sequence):
        h, by_y = sequence
        _, back = jax.vjp(lambda w: stack(w, h), weights)
        return jax.tree.map(lambda total, term: total + term.astype(jnp.float32), so_far, back(by_y)[0]), None

    none_yet = {name: jnp.zeros(w.shape, jnp.float32) for name, w in weights.items()}
    by_weights, _ = lax.scan(take, none_yet, (x, dy))
    gradients = [by_weights[name].astype(jnp.bfloat16).astype(jnp.float32) for name in NAMES]
    new = [
        adamw(w.astype(jnp.float32), m, v, g)
        for w, m, v, g in zip((w_gate, w_up, w_down), (m_w_gate, m_w_up, m_w_down), (v_w_gate, v_w_up, v_w_down), gradients, strict=True)
    ]
    return tuple(one[which] for which in range(3) for one in new)
```

```python
import jax
import jax.numpy as jnp
from jax import lax
from jax.experimental import pallas as pl
from jax.experimental.pallas import tpu as pltpu
from jax.sharding import PartitionSpec as P

F32, BF16 = jnp.float32, jnp.bfloat16
AXES = "dp"


DIMS = {"x": 16, "y": 8, "b": 4, "a": 2, "c": 1}
LEAD = "xyba"
PARTS = {
    2816: ((0, 1152, "xyab"), (1152, 2304, "yxab"), (2304, 2816, "abxy")),
    1024: ((0, 384, "xyab"), (384, 768, "yxab"), (768, 1024, "abyx")),
}
STEP = {32: 384, 88: 128}


def place():
    me = lax.axis_index(AXES)
    own = {d: (me // s) % 2 for d, s in DIMS.items()}
    peer = {d: me + (1 - 2 * own[d]) * s for d, s in DIMS.items()}
    return own, peer


def greet(peer):
    barrier = pltpu.get_barrier_semaphore()
    for d in DIMS:
        pl.semaphore_signal(barrier, inc=1, device_id={AXES: peer[d]}, device_id_type=pl.DeviceIdType.MESH)
    pl.semaphore_wait(barrier, len(DIMS))


def remote(src, dst, sems, n, target):
    return pltpu.make_async_remote_copy(
        src_ref=src, dst_ref=dst, send_sem=sems[0].at[n], recv_sem=sems[1].at[n], device_id={AXES: target}, device_id_type=pl.DeviceIdType.MESH
    )


def steps_of(lo, hi, rows):
    step = STEP[rows]
    return [(at, min(step, hi - at)) for at in range(lo, hi, step)]


def in_turn(steps, count):
    return sorted(((k, i) for k in range(steps) for i in range(count)), key=lambda at: 1.5 * at[0] + at[1])


class Scatter:
    def __init__(self, grad, held, came, later, out, sems, local, first, own, peer):
        self.grad, self.held, self.came, self.later, self.out = grad, held, came, later, out
        self.own, self.peer = own, peer
        self.rows, self.cols = grad.shape[-2:]
        self.parts = PARTS[self.cols]
        self.copies, n = {}, first
        for p, (lo, hi, order) in enumerate(self.parts):
            for half in range(2):
                at = tuple((1 - own[d] if half == 0 else own[d]) if d == order[0] else slice(None) for d in LEAD)
                here = at + (slice(None), pl.ds(lo, hi - lo))
                mine, theirs = at + (own["c"], slice(None), pl.ds(lo, hi - lo)), at + (1 - own["c"], slice(None), pl.ds(lo, hi - lo))
                self.copies["c", p, half] = remote(grad.at[theirs], came.at[here], sems, n, peer["c"])
                self.copies["own", p, half] = pltpu.make_async_copy(grad.at[mine], held.at[here], local.at[n])
                n += 1
            for k, d in enumerate(order):
                at = tuple(own[e] if e in order[:k] else 1 - own[e] if e == d else slice(None) for e in LEAD)
                self.copies[k, p] = remote(held.at[at + (slice(None), pl.ds(lo, hi - lo))], later[p][k], sems, n, peer[d])
                n += 1
        self.used = n - first

    def begin(self, half):
        for p in range(len(self.parts)):
            self.copies["c", p, half].start()
            self.copies["own", p, half].start()

    def add(self, p, k):
        lo, hi, order = self.parts[p]
        free = order[k + 1 :]

        def block(i, _):
            at = {}
            for n, e in enumerate(order):
                at[e] = self.own[e] if n < k else 1 - self.own[e] if n == k else (i // 2 ** (len(order) - 1 - n)) % 2
            lead = tuple(at[e] for e in LEAD)
            for c, size in steps_of(lo, hi, self.rows):
                here = lead + (slice(None), pl.ds(c, size))
                total = self.held[here].astype(F32) + self.came[here].astype(F32)
                for j in range(min(k, len(order))):
                    inner = tuple(at[e] for e in LEAD if e in order[j + 1 :])
                    total = total + self.later[p][j][inner + (slice(None), pl.ds(c - lo, size))].astype(F32)
                if k < len(order):
                    self.held[here] = total.astype(BF16)
                else:
                    self.out[:, pl.ds(c, size)] = total.astype(BF16)
            return 0

        if len(free) == 0:
            block(0, 0)
        else:
            lax.fori_loop(0, 2 ** len(free), block, 0)

    def send(self, p, k):
        if k == 0:
            self.copies["c", p, 0].wait_recv()
            self.copies["own", p, 0].wait()
        else:
            if k == 1:
                self.copies["c", p, 1].wait_recv()
                self.copies["own", p, 1].wait()
            self.copies[k - 1, p].wait_recv()
        self.add(p, k)
        if k < 4:
            self.copies[k, p].start()

    def finish(self):
        for name, copy in self.copies.items():
            if name[0] != "own":
                copy.wait_send()


def copies_of(cols):
    return len(PARTS[cols]) * 6


def later_shapes(rows, cols):
    return [[pltpu.VMEM((2,) * (3 - k) + (rows, hi - lo), BF16) for k in range(4)] for lo, hi, _ in PARTS[cols]]


def scatter(grads, collective_id):
    shapes = [g.shape for g in grads]
    shapes = [(s[0] // 32, s[1]) for s in shapes]
    count = len(shapes)

    def kernel(*refs):
        refs = list(refs)
        ins, outs = refs[:count], refs[count : 2 * count]
        held, came, later, sems, local = refs[2 * count :]
        own, peer = place()
        greet(peer)
        work, n = [], 0
        for i in range(count):
            work.append(Scatter(ins[i], held[i], came[i], later[i], outs[i], sems, local, n, own, peer))
            n += work[-1].used
        for half in range(2):
            for w in work:
                w.begin(half)
        for k, i in in_turn(5, count):
            for p in range(len(work[i].parts)):
                work[i].send(p, k)
        for w in work:
            w.finish()

    total = sum(copies_of(c) for _, c in shapes)
    return pl.pallas_call(
        kernel,
        name="scatter",
        out_shape=[jax.ShapeDtypeStruct(s, BF16) for s in shapes],
        in_specs=[pl.BlockSpec(memory_space=pl.ANY)] * count,
        out_specs=[pl.BlockSpec(memory_space=pltpu.VMEM)] * count,
        scratch_shapes=[
            [pltpu.VMEM((2, 2, 2, 2) + s, BF16) for s in shapes],
            [pltpu.VMEM((2, 2, 2, 2) + s, BF16) for s in shapes],
            [later_shapes(*s) for s in shapes],
            [pltpu.SemaphoreType.DMA((total,)), pltpu.SemaphoreType.DMA((total,))],
            pltpu.SemaphoreType.DMA((total,)),
        ],
        compiler_params=pltpu.CompilerParams(collective_id=collective_id, has_side_effects=True, vmem_limit_bytes=60 * 2**20),
    )(*(g.reshape((2,) * 5 + s) for g, s in zip(grads, shapes)))


def gather(blocks, collective_id):
    count = len(blocks)
    layers = blocks[0].shape[0]
    total = layers * sum(len(PARTS[b.shape[2]]) * 5 for b in blocks)

    def kernel(*refs):
        ins, outs = refs[:count], refs[count : 2 * count]
        send, recv, local = refs[2 * count :]
        own, peer = place()
        mine = tuple(own[e] for e in LEAD)
        every = slice(None)
        keep = [pltpu.make_async_copy(ins[i], outs[i].at[(every,) + mine + (own["c"],)], local.at[i]) for i in range(count)]
        for copy in keep:
            copy.start()
        greet(peer)
        copies, n = {}, 0
        units = [(layer, i) for layer in reversed(range(layers)) for i in range(count)]
        for u, (layer, i) in enumerate(units):
            for p, (lo, hi, order) in enumerate(PARTS[outs[i].shape[-1]]):
                cols = (every, pl.ds(lo, hi - lo))
                for k, d in enumerate(order[::-1] + "c"):
                    got = order[::-1][:k]
                    at = (layer,) + tuple(every if e in got else own[e] for e in LEAD) + (own["c"],) + cols
                    src = ins[i].at[(layer,) + cols] if k == 0 else outs[i].at[at]
                    copies[u, p, k] = remote(src, outs[i].at[at], (send, recv), n, peer[d])
                    n += 1
        kept = set()
        for k, u in in_turn(5, len(units)):
            i = units[u][1]
            if k == 1 and i not in kept:
                kept.add(i)
                keep[i].wait()
            for p in range(len(PARTS[outs[i].shape[-1]])):
                if k:
                    copies[u, p, k - 1].wait_recv()
                copies[u, p, k].start()
        for (u, p, k), copy in copies.items():
            if k == 4:
                copy.wait_recv()
            copy.wait_send()

    outs = pl.pallas_call(
        kernel,
        name="gather",
        out_shape=[jax.ShapeDtypeStruct((layers,) + (2,) * 5 + b.shape[1:], BF16) for b in blocks],
        in_specs=[pl.BlockSpec(memory_space=pl.ANY)] * count,
        out_specs=[pl.BlockSpec(memory_space=pl.ANY)] * count,
        scratch_shapes=[pltpu.SemaphoreType.DMA((total,)), pltpu.SemaphoreType.DMA((total,)), pltpu.SemaphoreType.DMA((count,))],
        compiler_params=pltpu.CompilerParams(collective_id=collective_id, has_side_effects=True),
    )(*blocks)
    return [o.reshape(layers, -1, o.shape[-1]) for o in outs]


def dot(a, b, contract):
    return lax.dot_general(a, b, ((contract[:1], contract[1:]), ((), ())), preferred_element_type=F32)


def norm_scale(h):
    wide = h.astype(F32)
    return lax.rsqrt(jnp.mean(wide**2, -1, keepdims=True) + 1e-6)


def adamw(w, m, v, g):
    m = 0.9 * m + 0.1 * g
    v = 0.95 * v + 0.05 * g * g
    step = m * lax.rsqrt(v + 1e-8) + 0.1 * w
    return (w - 0.02 * step).astype(BF16), m, v


def silu_parts(gate):
    s = jax.nn.sigmoid(gate)
    return gate * s, s * (1 + gate * (1 - s))


def body(x, dy, wg, wu, wd, mg, mu, md, vg, vu, vd):
    x, dy = x[0], dy[0]
    a0 = (x.astype(F32) * norm_scale(x)).astype(BF16)
    g0 = dot(a0, wg[0], (1, 0))
    u0 = dot(a0, wu[0], (1, 0))
    p0 = (jax.nn.silu(g0) * u0).astype(BF16)
    h1 = x + dot(p0, wd[0], (1, 0)).astype(BF16)
    r1 = norm_scale(h1)
    a1 = (h1.astype(F32) * r1).astype(BF16)
    g1 = dot(a1, wg[1], (1, 0))
    u1 = dot(a1, wu[1], (1, 0))

    def back(a, p, g, u, d, wdl):
        dp = dot(d, wdl, (1, 1)).astype(BF16).astype(F32)
        s, ds = silu_parts(g)
        dwd = dot(p, d, (0, 0)).astype(BF16)
        dg = (dp * u * ds).astype(BF16)
        du = (dp * s).astype(BF16)
        return dg, du, dot(a, dg, (0, 0)).astype(BF16), dot(a, du, (0, 0)).astype(BF16), dwd

    p1 = (jax.nn.silu(g1) * u1).astype(BF16)
    dg1, du1, dwg1, dwu1, dwd1 = back(a1, p1, g1, u1, dy, wd[1])
    da1 = (dot(dg1, wg[1], (1, 1)).astype(BF16) + dot(du1, wu[1], (1, 1)).astype(BF16)).astype(F32)
    wide = h1.astype(F32)
    inner = jnp.sum(da1 * wide, -1, keepdims=True) / wide.shape[-1]
    dnorm = (da1 * r1 - wide * (r1 * r1 * r1) * inner).astype(BF16)
    dh1 = dy + dnorm
    dg0, du0, dwg0, dwu0, dwd0 = back(a0, p0, g0, u0, dh1, wd[0])
    i = lax.axis_index(AXES)
    sums1 = scatter([dwd1, dwg1, dwu1], 0)
    sums0 = scatter([dwd0, dwg0, dwu0], 1)
    new = []
    for w, m, v, one, two in ((wd, md, vd, sums0[0], sums1[0]), (wg, mg, vg, sums0[1], sums1[1]), (wu, mu, vu, sums0[2], sums1[2])):
        n = m.shape[1]
        g = jnp.stack([one, two]).astype(F32)
        mine = lax.dynamic_slice_in_dim(w, i * n, n, 1).astype(F32)
        new.append(adamw(mine, m, v, g))
    nd, ng, nu = gather([n[0] for n in new], 2)
    down, gate, up = new
    return ng, nu, nd, gate[1], up[1], down[1], gate[2], up[2], down[2]


def solution(mesh):
    whole, seq, part = P(None, None, None), P(("rep", "dp"), None, None), P(None, "dp", None)
    outw, outm = P("rep", None, None), P("rep", "dp", None)
    return jax.shard_map(body, mesh=mesh, in_specs=(seq, seq) + (whole,) * 3 + (part,) * 6, out_specs=(outw,) * 3 + (outm,) * 6, check_vma=False)
```

```python
import functools

import jax
import jax.numpy as jnp
from jax import lax
from jax.experimental import pallas as pl
from jax.experimental.pallas import tpu as pltpu
from jax.sharding import PartitionSpec as P

F32, BF16 = jnp.float32, jnp.bfloat16
AXES = "dp"


DIMS = {"x": 16, "y": 8, "b": 4, "a": 2, "c": 1}
LEAD = "xyba"
PARTS = {
    2816: ((0, 1152, "xyab"), (1152, 2304, "yxab"), (2304, 2816, "abxy")),
    1024: ((0, 384, "xyab"), (384, 768, "yxab"), (768, 1024, "abyx")),
}
STEP = {32: 384, 88: 128}


def place():
    me = lax.axis_index(AXES)
    own = {d: (me // s) % 2 for d, s in DIMS.items()}
    peer = {d: me + (1 - 2 * own[d]) * s for d, s in DIMS.items()}
    return own, peer


def greet(peer):
    barrier = pltpu.get_barrier_semaphore()
    for d in DIMS:
        pl.semaphore_signal(barrier, inc=1, device_id={AXES: peer[d]}, device_id_type=pl.DeviceIdType.MESH)
    pl.semaphore_wait(barrier, len(DIMS))


def remote(src, dst, sems, n, target):
    return pltpu.make_async_remote_copy(
        src_ref=src, dst_ref=dst, send_sem=sems[0].at[n], recv_sem=sems[1].at[n], device_id={AXES: target}, device_id_type=pl.DeviceIdType.MESH
    )


def steps_of(lo, hi, rows):
    step = STEP[rows]
    return [(at, min(step, hi - at)) for at in range(lo, hi, step)]


def in_turn(steps, count):
    return sorted(((k, i) for k in range(steps) for i in range(count)), key=lambda at: 1.5 * at[0] + at[1])


class Scatter:
    def __init__(self, grad, held, came, later, out, sems, local, first, own, peer):
        self.grad, self.held, self.came, self.later, self.out = grad, held, came, later, out
        self.own, self.peer = own, peer
        self.rows, self.cols = grad.shape[-2:]
        self.parts = PARTS[self.cols]
        self.copies, n = {}, first
        for p, (lo, hi, order) in enumerate(self.parts):
            for half in range(2):
                at = tuple((1 - own[d] if half == 0 else own[d]) if d == order[0] else slice(None) for d in LEAD)
                here = at + (slice(None), pl.ds(lo, hi - lo))
                mine, theirs = at + (own["c"], slice(None), pl.ds(lo, hi - lo)), at + (1 - own["c"], slice(None), pl.ds(lo, hi - lo))
                self.copies["c", p, half] = remote(grad.at[theirs], came.at[here], sems, n, peer["c"])
                self.copies["own", p, half] = pltpu.make_async_copy(grad.at[mine], held.at[here], local.at[n])
                n += 1
            for k, d in enumerate(order):
                at = tuple(own[e] if e in order[:k] else 1 - own[e] if e == d else slice(None) for e in LEAD)
                self.copies[k, p] = remote(held.at[at + (slice(None), pl.ds(lo, hi - lo))], later[p][k], sems, n, peer[d])
                n += 1
        self.used = n - first

    def begin(self, half):
        for p in range(len(self.parts)):
            self.copies["c", p, half].start()
            self.copies["own", p, half].start()

    def add(self, p, k):
        lo, hi, order = self.parts[p]
        free = order[k + 1 :]

        def block(i, _):
            at = {}
            for n, e in enumerate(order):
                at[e] = self.own[e] if n < k else 1 - self.own[e] if n == k else (i // 2 ** (len(order) - 1 - n)) % 2
            lead = tuple(at[e] for e in LEAD)
            for c, size in steps_of(lo, hi, self.rows):
                here = lead + (slice(None), pl.ds(c, size))
                total = self.held[here].astype(F32) + self.came[here].astype(F32)
                for j in range(min(k, len(order))):
                    inner = tuple(at[e] for e in LEAD if e in order[j + 1 :])
                    total = total + self.later[p][j][inner + (slice(None), pl.ds(c - lo, size))].astype(F32)
                if k < len(order):
                    self.held[here] = total.astype(BF16)
                else:
                    self.out[:, pl.ds(c, size)] = total.astype(BF16)
            return 0

        if len(free) == 0:
            block(0, 0)
        else:
            lax.fori_loop(0, 2 ** len(free), block, 0)

    def send(self, p, k):
        if k == 0:
            self.copies["c", p, 0].wait_recv()
            self.copies["own", p, 0].wait()
        else:
            if k == 1:
                self.copies["c", p, 1].wait_recv()
                self.copies["own", p, 1].wait()
            self.copies[k - 1, p].wait_recv()
        self.add(p, k)
        if k < 4:
            self.copies[k, p].start()

    def finish(self):
        for name, copy in self.copies.items():
            if name[0] != "own":
                copy.wait_send()


def copies_of(cols):
    return len(PARTS[cols]) * 6


def later_shapes(rows, cols):
    return [[pltpu.VMEM((2,) * (3 - k) + (rows, hi - lo), BF16) for k in range(4)] for lo, hi, _ in PARTS[cols]]


class Gather:
    def __init__(self, block, out, sems, local, first, own, peer):
        rows, cols = block.shape
        every = slice(None)
        self.parts = PARTS[cols]
        self.keep = pltpu.make_async_copy(block, out.at[tuple(own[e] for e in LEAD) + (own["c"],)], local.at[first])
        self.copies, n = {}, first
        for p, (lo, hi, order) in enumerate(self.parts):
            at_cols = (every, pl.ds(lo, hi - lo))
            for k, d in enumerate(order[::-1] + "c"):
                got = order[::-1][:k]
                at = tuple(every if e in got else own[e] for e in LEAD) + (own["c"],) + at_cols
                self.copies[k, p] = remote(block.at[at_cols] if k == 0 else out.at[at], out.at[at], sems, n, peer[d])
                n += 1
        self.used = n - first

    def begin(self, half):
        if half == 0:
            self.keep.start()

    def send(self, p, k):
        if k == 1 and p == 0:
            self.keep.wait()
        if k:
            self.copies[k - 1, p].wait_recv()
        self.copies[k, p].start()

    def finish(self):
        for (k, _), copy in self.copies.items():
            if k == 4:
                copy.wait_recv()
            copy.wait_send()


def host(name, body, steps, ins, outs, args, scratch=(), grads=(), blocks=(), collective_id=None, flops=0):
    grads = [g.reshape((2,) * 5 + (g.shape[0] // 32, g.shape[1])) for g in grads]
    shapes = [g.shape[5:] for g in grads]
    counts = [len(ins), len(grads), len(blocks), len(outs), len(grads), len(blocks), len(scratch)]
    total = sum(copies_of(s[1]) for s in shapes) + sum(5 * len(PARTS[b.shape[1]]) for b in blocks)
    anywhere, units_count = pl.BlockSpec(memory_space=pl.ANY), len(grads) + len(blocks)

    def kernel(*refs):
        refs, groups = list(refs), []
        for n in counts:
            groups.append(refs[:n])
            refs = refs[n:]
        mine, grad_refs, block_refs, results, sums, gathered, own_scratch = groups
        step = pl.program_id(0)
        if units_count:
            held, came, later, sems, local = refs
            own, peer = place()
            work, n = [], 0
            for i in range(len(grads)):
                work.append(Scatter(grad_refs[i], held[i], came[i], later[i], sums[i], sems, local, n, own, peer))
                n += work[-1].used
            for i in range(len(blocks)):
                work.append(Gather(block_refs[i], gathered[i], sems, local, n, own, peer))
                n += work[-1].used
            turns = in_turn(5, units_count)

            def begin():
                greet(peer)
                for half in range(2):
                    for w in work:
                        w.begin(half)

            def at(which):
                for k, i in which:
                    for p in range(len(work[i].parts)):
                        work[i].send(p, k)

            def finish():
                for w in work:
                    w.finish()

            if steps == 1:
                begin()
                at(turns)
                finish()
            else:
                pl.when(step == 0)(begin)
                when = {}
                for n, turn in enumerate(turns):
                    when.setdefault(1 + n * (steps - 1) // len(turns), []).append(turn)
                for n, which in when.items():
                    pl.when(step == n)(functools.partial(at, which))
        if body is not None:
            body(step, *mine, *results, *own_scratch)
        if units_count and steps > 1:
            pl.when(step == steps - 1)(finish)

    comm_scratch = []
    if units_count:
        comm_scratch = [
            [pltpu.VMEM((2, 2, 2, 2) + s, BF16) for s in shapes],
            [pltpu.VMEM((2, 2, 2, 2) + s, BF16) for s in shapes],
            [later_shapes(*s) for s in shapes],
            [pltpu.SemaphoreType.DMA((total,)), pltpu.SemaphoreType.DMA((total,))],
            pltpu.SemaphoreType.DMA((total,)),
        ]
    params = dict(collective_id=collective_id, has_side_effects=True) if units_count else {}
    whole = lambda s: pl.BlockSpec(s, lambda i: (0, 0))
    results = pl.pallas_call(
        kernel,
        name=name,
        grid=(steps,),
        in_specs=list(ins) + [anywhere] * units_count,
        out_specs=[o[0] for o in outs] + [whole(s) for s in shapes] + [anywhere] * len(blocks),
        out_shape=[jax.ShapeDtypeStruct(*o[1:]) for o in outs]
        + [jax.ShapeDtypeStruct(s, BF16) for s in shapes]
        + [jax.ShapeDtypeStruct((2,) * 5 + b.shape, BF16) for b in blocks],
        scratch_shapes=list(scratch) + comm_scratch,
        compiler_params=pltpu.CompilerParams(vmem_limit_bytes=62 * 2**20, dimension_semantics=("arbitrary",), **params),
        cost_estimate=pl.CostEstimate(flops=flops + 10**9, bytes_accessed=60 * 2**20, transcendentals=0),
    )(*args, *grads, *blocks)
    a, b = len(outs), len(outs) + len(grads)
    return results[:a], results[a:b], [r.reshape(-1, r.shape[-1]) for r in results[b:]]


def dot(a, b, contract):
    return lax.dot_general(a, b, ((contract[:1], contract[1:]), ((), ())), preferred_element_type=F32)


def norm_scale(h):
    wide = h.astype(F32)
    return lax.rsqrt(jnp.mean(wide**2, -1, keepdims=True) + 1e-6)


def adamw(w, m, v, g):
    m = 0.9 * m + 0.1 * g
    v = 0.95 * v + 0.05 * g * g
    step = m * lax.rsqrt(v + 1e-8) + 0.1 * w
    return (w - 0.02 * step).astype(BF16), m, v


def silu_parts(gate):
    s = 0.5 * jnp.tanh(0.5 * gate) + 0.5
    y = gate * s
    return y, s + y * (1 - s)


TM = 128
CHUNKS = [(at, min(512, 2816 - at)) for at in range(0, 2816, 512)]
HALVES = [(0, 512), (512, 512)]


def fetch(refs, bufs, sems):
    return [pltpu.make_async_copy(r, b, sems.at[n]) for n, (r, b) in enumerate(zip(refs, bufs))]


def scale_of(h):
    wide = h.astype(F32)
    return wide, lax.rsqrt(jnp.mean(wide * wide, -1, keepdims=True) + 1e-6)


def forth_kernel(x, dy, wg, wu, wd, a0o, g0o, u0o, p0o, h1o, a1o, p1o, dg1o, du1o, wg0, wu0, wd0, wg1, wu1, wd1, sems):
    bufs = (wg0, wu0, wd0, wd1, wg1, wu1)
    copies = fetch([wg.at[0], wu.at[0], wd.at[0], wd.at[1], wg.at[1], wu.at[1]], bufs, sems)
    first = pl.program_id(0) == 0

    def need(*which):
        @pl.when(first)
        def _():
            for n in which:
                copies[n].wait()

    @pl.when(first)
    def _():
        for copy in copies:
            copy.start()

    wide, r = scale_of(x[...])
    a = (wide * r).astype(BF16)
    a0o[...] = a
    need(0, 1)
    for at, size in CHUNKS:
        cols = pl.ds(at, size)
        g = dot(a, wg0[:, cols], (1, 0))
        u = dot(a, wu0[:, cols], (1, 0))
        g0o[:, cols] = g
        u0o[:, cols] = u
        p0o[:, cols] = (silu_parts(g)[0] * u).astype(BF16)
    need(2)
    for at, size in HALVES:
        cols = pl.ds(at, size)
        h1o[:, cols] = x[:, cols] + dot(p0o[...], wd0[:, cols], (1, 0)).astype(BF16)
    wide, r = scale_of(h1o[...])
    a = (wide * r).astype(BF16)
    a1o[...] = a
    need(3, 4, 5)
    d = dy[...]
    for at, size in CHUNKS:
        cols = pl.ds(at, size)
        g = dot(a, wg1[:, cols], (1, 0))
        u = dot(a, wu1[:, cols], (1, 0))
        dp = dot(d, wd1[cols, :], (1, 1)).astype(BF16).astype(F32)
        s, ds = silu_parts(g)
        p1o[:, cols] = (s * u).astype(BF16)
        dg1o[:, cols] = (dp * u * ds).astype(BF16)
        du1o[:, cols] = (dp * s).astype(BF16)


def forth(x, dy, wg, wu, wd):
    tokens, d = x.shape
    ff = wg.shape[2]
    spec = lambda n: pl.BlockSpec((TM, n), lambda i: (i, 0))
    outs = [(d, BF16), (ff, F32), (ff, F32), (ff, BF16), (d, BF16), (d, BF16), (ff, BF16), (ff, BF16), (ff, BF16)]
    return pl.pallas_call(
        forth_kernel,
        name="forth",
        grid=(tokens // TM,),
        in_specs=[spec(d), spec(d)] + [pl.BlockSpec(memory_space=pl.ANY)] * 3,
        out_specs=[spec(n) for n, _ in outs],
        out_shape=[jax.ShapeDtypeStruct((tokens, n), t) for n, t in outs],
        scratch_shapes=[pltpu.VMEM(s, BF16) for s in ((d, ff), (d, ff), (ff, d)) * 2] + [pltpu.SemaphoreType.DMA((6,))],
        compiler_params=pltpu.CompilerParams(vmem_limit_bytes=62 * 2**20, dimension_semantics=("arbitrary",)),
        cost_estimate=pl.CostEstimate(flops=12 * tokens * d * ff, bytes_accessed=180 * 2**20, transcendentals=2 * tokens * ff),
    )(x, dy, wg, wu, wd)


def back_body(step, dg1, du1, dy, h1, g0, u0, wg, wu, wd, dh1o, dg0o, du0o, wg1, wu1, wd0, sems):
    copies = fetch([wg.at[1], wu.at[1], wd.at[0]], (wg1, wu1, wd0), sems)

    @pl.when(step == 0)
    def _():
        for copy in copies:
            copy.start()
        for copy in copies:
            copy.wait()

    by_gate = dot(dg1[...], wg1[...], (1, 1)).astype(BF16)
    by_up = dot(du1[...], wu1[...], (1, 1)).astype(BF16)
    da = (by_gate + by_up).astype(F32)
    wide, r = scale_of(h1[...])
    inner = jnp.mean(da * wide, -1, keepdims=True)
    dh1o[...] = dy[...] + (da * r - wide * (r * r * r) * inner).astype(BF16)
    d = dh1o[...]
    for at, size in CHUNKS:
        cols = pl.ds(at, size)
        dp = dot(d, wd0[cols, :], (1, 1)).astype(BF16).astype(F32)
        s, ds = silu_parts(g0[:, cols])
        dg0o[:, cols] = (dp * u0[:, cols] * ds).astype(BF16)
        du0o[:, cols] = (dp * s).astype(BF16)


def back(dg1, du1, dy, h1, g0, u0, wg, wu, wd, **beside):
    tokens, d = dy.shape
    ff = wg.shape[2]
    tm = 256
    spec = lambda n: pl.BlockSpec((tm, n), lambda i: (i, 0))
    return host(
        "back",
        back_body,
        tokens // tm,
        [spec(n) for n in (ff, ff, d, d, ff, ff)] + [pl.BlockSpec(memory_space=pl.ANY)] * 3,
        [(spec(n), (tokens, n), BF16) for n in (d, ff, ff)],
        (dg1, du1, dy, h1, g0, u0, wg, wu, wd),
        [pltpu.VMEM(s, BF16) for s in ((d, ff), (d, ff), (ff, d))] + [pltpu.SemaphoreType.DMA((3,))],
        flops=6 * tokens * d * ff,
        **beside,
    )


def outers(p, d, a, wide, **beside):
    tokens, tile = a.shape[0], 256
    ff, dim = wide[0].shape[1], a.shape[1]
    tiles = ff // tile
    downs = tiles if p is not None else 0
    steps = downs + tiles * len(wide)
    ins, outs, args, scratch = [], [], [], []
    if p is not None:
        ins += [pl.BlockSpec((tokens, tile), lambda i: (0, jnp.minimum(i, tiles - 1))), pl.BlockSpec((tokens, dim), lambda i: (0, 0))]
        outs.append((pl.BlockSpec((tile, dim), lambda i: (jnp.minimum(i, tiles - 1), 0)), (ff, dim), BF16))
        args += [p, d]
    if wide:
        ins.append(pl.BlockSpec((tokens, dim), lambda i: (0, 0)))
        args.append(a)
        scratch.append(pltpu.VMEM((dim, tokens), BF16))

    def column(first):
        return lambda i: (0, jnp.clip(i - first, 0, tiles - 1))

    for n, w in enumerate(wide):
        ins.append(pl.BlockSpec((tokens, tile), column(downs + n * tiles)))
        outs.append((pl.BlockSpec((dim, tile), column(downs + n * tiles)), (dim, ff), BF16))
        args.append(w)

    def work(step, *refs):
        refs = list(refs)
        if p is not None:
            p_ref, d_ref = refs[:2]
            refs = refs[2:]
        a_ref, w_refs, o_refs, turned = refs[0], refs[1 : 1 + len(wide)], refs[1 + len(wide) : -1], refs[-1]

        if p is not None:

            @pl.when(step < downs)
            def _():
                for at, size in HALVES:
                    o_refs[0][:, pl.ds(at, size)] = dot(p_ref[...], d_ref[:, pl.ds(at, size)], (0, 0)).astype(BF16)

        @pl.when(step == downs)
        def _():
            for at in range(0, tokens, 512):
                turned[:, pl.ds(at, 512)] = a_ref[pl.ds(at, 512), :].T

        for n in range(len(wide)):
            first, w_ref, o_ref = downs + n * tiles, w_refs[n], o_refs[n - len(wide)]

            @pl.when((step >= first) & (step < first + tiles))
            def _():
                o_ref[...] = dot(turned[...], w_ref[...], (1, 0)).astype(BF16)

    return host("outers", work, steps, ins, outs, args, scratch, flops=2 * tokens * tile * dim * steps, **beside)


def outer(a, b, tile=256):
    tokens, m = a.shape
    n = b.shape[1]

    def work(step, a_ref, b_ref, o):
        for at, size in HALVES:
            o[:, pl.ds(at, size)] = dot(a_ref[...], b_ref[:, pl.ds(at, size)], (0, 0)).astype(BF16)

    ins = [pl.BlockSpec((tokens, tile), lambda i: (0, i)), pl.BlockSpec((tokens, n), lambda i: (0, 0))]
    outs = [(pl.BlockSpec((tile, n), lambda i: (i, 0)), (m, n), BF16)]
    return host("outer", work, m // tile, ins, outs, (a, b), flops=2 * tokens * m * n)[0][0]


def body(x, dy, wg, wu, wd, mg, mu, md, vg, vu, vd):
    x, dy = x[0], dy[0]
    i = lax.axis_index(AXES)

    def update(layer, w, m, v, g):
        rows = m.shape[1]
        mine = lax.dynamic_slice_in_dim(w[layer], i * rows, rows, 0).astype(F32)
        return adamw(mine, m[layer], v[layer], g.astype(F32))

    a0, g0, u0, p0, h1, a1, p1, dg1, du1 = forth(x, dy, wg, wu, wd)
    dwd1 = outer(p1, dy)
    (dwg1, dwu1), (sd1,), _ = outers(None, None, a1, [dg1, du1], grads=[dwd1], collective_id=0)
    nd1 = update(1, wd, md, vd, sd1)
    (dh1, dg0, du0), (sg1, su1), _ = back(dg1, du1, dy, h1, g0, u0, wg, wu, wd, grads=[dwg1, dwu1], collective_id=1)
    ng1 = update(1, wg, mg, vg, sg1)
    nu1 = update(1, wu, mu, vu, su1)
    (dwd0, dwg0, dwu0), _, (fd1, fg1) = outers(p0, dh1, a0, [dg0, du0], blocks=[nd1[0], ng1[0]], collective_id=2)
    _, (sd0, sg0, su0), (fu1,) = host("ends", None, 1, [], [], (), grads=[dwd0, dwg0, dwu0], blocks=[nu1[0]], collective_id=3)
    nd0, ng0, nu0 = update(0, wd, md, vd, sd0), update(0, wg, mg, vg, sg0), update(0, wu, mu, vu, su0)
    _, _, (fd0, fg0, fu0) = host("last", None, 1, [], [], (), blocks=[nd0[0], ng0[0], nu0[0]], collective_id=4)
    stacked = [jnp.stack(pair) for pair in ((fg0, fg1), (fu0, fu1), (fd0, fd1))]
    for which in (1, 2):
        stacked += [jnp.stack([a[which], b[which]]) for a, b in ((ng0, ng1), (nu0, nu1), (nd0, nd1))]
    return tuple(stacked)


def solution(mesh):
    whole, seq, part = P(None, None, None), P(("rep", "dp"), None, None), P(None, "dp", None)
    outw, outm = P("rep", None, None), P("rep", "dp", None)
    return jax.shard_map(body, mesh=mesh, in_specs=(seq, seq) + (whole,) * 3 + (part,) * 6, out_specs=(outw,) * 3 + (outm,) * 6, check_vma=False)
```

```python
import functools

import jax
import jax.numpy as jnp
from jax import lax
from jax.experimental import pallas as pl
from jax.experimental.pallas import tpu as pltpu
from jax.sharding import PartitionSpec as P

F32, BF16 = jnp.float32, jnp.bfloat16
AXES = "dp"


DIMS = {"x": 16, "y": 8, "b": 4, "a": 2, "c": 1}
LEAD = "xyba"
SUM_PARTS = {
    "d1": ((0, 384, "xyab"), (384, 768, "yxab"), (768, 1024, "abxy")),
    "g1": ((0, 1152, "xyab"), (1152, 2304, "yxab"), (2304, 2816, "abxy")),
    "u1": ((0, 1024, "xyab"), (1024, 2048, "yxab"), (2048, 2816, "abyx")),
    "d0": ((0, 512, "xyab"), (512, 1024, "yxab")),
    "g0": ((0, 1024, "xyab"), (1024, 2048, "yxab"), (2048, 2816, "abxy")),
    "u0": (
        (0, 640, "xyab"),
        (640, 1152, "yxab"),
        (1152, 1536, "axyb"),
        (1536, 1920, "ayxb"),
        (1920, 2432, "abyx"),
        (2432, 2816, "abxy"),
    ),
}
NEW_PARTS = {
    "d": ((0, 384, "xyab"), (384, 768, "yxab"), (768, 1024, "axyb")),
    "g": ((0, 1024, "xyab"), (1024, 1920, "yxab"), (1920, 2432, "axyb"), (2432, 2816, "ayxb")),
    "u": ((0, 896, "xyab"), (896, 1792, "yxab"), (1792, 2304, "axyb"), (2304, 2816, "ayxb")),
}
STEP = {32: 384, 88: 128}


def place():
    me = lax.axis_index(AXES)
    own = {d: (me // s) % 2 for d, s in DIMS.items()}
    peer = {d: me + (1 - 2 * own[d]) * s for d, s in DIMS.items()}
    return own, peer


def greet(peer):
    barrier = pltpu.get_barrier_semaphore()
    for d in DIMS:
        pl.semaphore_signal(barrier, inc=1, device_id={AXES: peer[d]}, device_id_type=pl.DeviceIdType.MESH)
    pl.semaphore_wait(barrier, len(DIMS))


def remote(src, dst, sems, n, target):
    return pltpu.make_async_remote_copy(
        src_ref=src, dst_ref=dst, send_sem=sems[0].at[n], recv_sem=sems[1].at[n], device_id={AXES: target}, device_id_type=pl.DeviceIdType.MESH
    )


def steps_of(lo, hi, rows):
    step = STEP[rows]
    return [(at, min(step, hi - at)) for at in range(lo, hi, step)]


def in_turn(chains):
    turns = [(k, i, p) for k in range(5) for i, parts in enumerate(chains) for p in range(len(parts))]
    return sorted(turns, key=lambda at: 1.5 * at[0] + at[1] * (0.3 if chains[at[1]][at[2]][2][0] == "a" else 1.0))


class Scatter:
    def __init__(self, parts, grad, held, came, later, out, sems, local, first, own, peer):
        self.grad, self.held, self.came, self.later, self.out = grad, held, came, later, out
        self.own, self.peer = own, peer
        self.rows, self.cols = grad.shape[-2:]
        self.parts = parts
        self.copies, n = {}, first
        for p, (lo, hi, order) in enumerate(self.parts):
            for half in range(2):
                at = tuple((1 - own[d] if half == 0 else own[d]) if d == order[0] else slice(None) for d in LEAD)
                here = at + (slice(None), pl.ds(lo, hi - lo))
                mine, theirs = at + (own["c"], slice(None), pl.ds(lo, hi - lo)), at + (1 - own["c"], slice(None), pl.ds(lo, hi - lo))
                self.copies["c", p, half] = remote(grad.at[theirs], came.at[here], sems, n, peer["c"])
                self.copies["own", p, half] = pltpu.make_async_copy(grad.at[mine], held.at[here], local.at[n])
                n += 1
            for k, d in enumerate(order):
                at = tuple(own[e] if e in order[:k] else 1 - own[e] if e == d else slice(None) for e in LEAD)
                self.copies[k, p] = remote(held.at[at + (slice(None), pl.ds(lo, hi - lo))], later[p][k], sems, n, peer[d])
                n += 1
        self.used = n - first

    def begin(self, half):
        for p in range(len(self.parts)):
            self.copies["c", p, half].start()
            self.copies["own", p, half].start()

    def add(self, p, k):
        lo, hi, order = self.parts[p]
        free = order[k + 1 :]

        def block(i, _):
            at = {}
            for n, e in enumerate(order):
                at[e] = self.own[e] if n < k else 1 - self.own[e] if n == k else (i // 2 ** (len(order) - 1 - n)) % 2
            lead = tuple(at[e] for e in LEAD)
            for c, size in steps_of(lo, hi, self.rows):
                here = lead + (slice(None), pl.ds(c, size))
                total = self.held[here].astype(F32) + self.came[here].astype(F32)
                for j in range(min(k, len(order))):
                    inner = tuple(at[e] for e in LEAD if e in order[j + 1 :])
                    total = total + self.later[p][j][inner + (slice(None), pl.ds(c - lo, size))].astype(F32)
                if k < len(order):
                    self.held[here] = total.astype(BF16)
                else:
                    self.out[:, pl.ds(c, size)] = total.astype(BF16)
            return 0

        if len(free) == 0:
            block(0, 0)
        else:
            lax.fori_loop(0, 2 ** len(free), block, 0)

    def send(self, p, k):
        if k == 0:
            self.copies["c", p, 0].wait_recv()
            self.copies["own", p, 0].wait()
        else:
            if k == 1:
                self.copies["c", p, 1].wait_recv()
                self.copies["own", p, 1].wait()
            self.copies[k - 1, p].wait_recv()
        self.add(p, k)
        if k < 4:
            self.copies[k, p].start()

    def finish(self):
        for name, copy in self.copies.items():
            if name[0] != "own":
                copy.wait_send()


def later_shapes(parts, rows):
    return [[pltpu.VMEM((2,) * (3 - k) + (rows, hi - lo), BF16) for k in range(4)] for lo, hi, _ in parts]


class Gather:
    def __init__(self, parts, block, out, sems, local, first, own, peer):
        rows, cols = block.shape
        every = slice(None)
        self.parts = parts
        self.kept = False
        self.keep = pltpu.make_async_copy(block, out.at[tuple(own[e] for e in LEAD) + (own["c"],)], local.at[first])
        self.copies, n = {}, first
        for p, (lo, hi, order) in enumerate(self.parts):
            at_cols = (every, pl.ds(lo, hi - lo))
            for k, d in enumerate(order[::-1] + "c"):
                got = order[::-1][:k]
                at = tuple(every if e in got else own[e] for e in LEAD) + (own["c"],) + at_cols
                self.copies[k, p] = remote(block.at[at_cols] if k == 0 else out.at[at], out.at[at], sems, n, peer[d])
                n += 1
        self.used = n - first

    def begin(self, half):
        if half == 0:
            self.keep.start()

    def send(self, p, k):
        if k == 1 and not self.kept:
            self.kept = True
            self.keep.wait()
        if k:
            self.copies[k - 1, p].wait_recv()
        self.copies[k, p].start()

    def finish(self):
        for (k, _), copy in self.copies.items():
            if k == 4:
                copy.wait_recv()
            copy.wait_send()


def host(name, body, steps, ins, outs, args, scratch=(), grads={}, blocks={}, collective_id=None, flops=0, ticks=1):
    chains = [SUM_PARTS[name] for name in grads] + [NEW_PARTS[name] for name in blocks]
    grads = [g.reshape((2,) * 5 + (g.shape[0] // 32, g.shape[1])) for g in grads.values()]
    blocks = list(blocks.values())
    shapes = [g.shape[5:] for g in grads]
    counts = [len(ins), len(grads), len(blocks), len(outs), len(grads), len(blocks), len(scratch)]
    total = sum((6 if n < len(grads) else 5) * len(parts) for n, parts in enumerate(chains))
    anywhere, units_count = pl.BlockSpec(memory_space=pl.ANY), len(grads) + len(blocks)

    def kernel(*refs):
        refs, groups = list(refs), []
        for n in counts:
            groups.append(refs[:n])
            refs = refs[n:]
        mine, grad_refs, block_refs, results, sums, gathered, own_scratch = groups
        step = pl.program_id(0)
        if units_count:
            held, came, later, sems, local = refs
            own, peer = place()
            work, n = [], 0
            for i in range(len(grads)):
                work.append(Scatter(chains[i], grad_refs[i], held[i], came[i], later[i], sums[i], sems, local, n, own, peer))
                n += work[-1].used
            for i in range(len(blocks)):
                work.append(Gather(chains[len(grads) + i], block_refs[i], gathered[i], sems, local, n, own, peer))
                n += work[-1].used
            turns = in_turn(chains)

            def begin():
                greet(peer)
                for half in range(2):
                    for w in work:
                        w.begin(half)

            def at(which):
                for k, i, p in which:
                    work[i].send(p, k)

            def finish():
                for w in work:
                    w.finish()

            when, slots = {}, steps * ticks
            for n, turn in enumerate(turns):
                when.setdefault(1 + n * (slots - 1) // len(turns), []).append(turn)

            def tick(j):
                if j == 0:
                    pl.when(step == 0)(begin)
                for n in sorted(when):
                    if n % ticks == j:
                        pl.when(step == n // ticks)(functools.partial(at, when[n]))

            if body is None:
                begin()
                at(turns)
                finish()
        else:
            tick = lambda j: None
        if body is not None:
            body(step, tick, *mine, *results, *own_scratch)
            if units_count:
                pl.when(step == steps - 1)(finish)

    comm_scratch = []
    if units_count:
        comm_scratch = [
            [pltpu.VMEM((2, 2, 2, 2) + s, BF16) for s in shapes],
            [pltpu.VMEM((2, 2, 2, 2) + s, BF16) for s in shapes],
            [later_shapes(parts, s[0]) for parts, s in zip(chains, shapes)],
            [pltpu.SemaphoreType.DMA((total,)), pltpu.SemaphoreType.DMA((total,))],
            pltpu.SemaphoreType.DMA((total,)),
        ]
    params = dict(collective_id=collective_id, has_side_effects=True) if units_count else {}
    whole = lambda s: pl.BlockSpec(s, lambda i: (0, 0))
    results = pl.pallas_call(
        kernel,
        name=name,
        grid=(steps,),
        in_specs=list(ins) + [anywhere] * units_count,
        out_specs=[o[0] for o in outs] + [whole(s) for s in shapes] + [anywhere] * len(blocks),
        out_shape=[jax.ShapeDtypeStruct(*o[1:]) for o in outs]
        + [jax.ShapeDtypeStruct(s, BF16) for s in shapes]
        + [jax.ShapeDtypeStruct((2,) * 5 + b.shape, BF16) for b in blocks],
        scratch_shapes=list(scratch) + comm_scratch,
        compiler_params=pltpu.CompilerParams(vmem_limit_bytes=62 * 2**20, dimension_semantics=("arbitrary",), **params),
        cost_estimate=pl.CostEstimate(flops=flops + 10**9, bytes_accessed=60 * 2**20, transcendentals=0),
    )(*args, *grads, *blocks)
    a, b = len(outs), len(outs) + len(grads)
    return results[:a], results[a:b], [r.reshape(-1, r.shape[-1]) for r in results[b:]]


def dot(a, b, contract):
    return lax.dot_general(a, b, ((contract[:1], contract[1:]), ((), ())), preferred_element_type=F32)


def norm_scale(h):
    wide = h.astype(F32)
    return lax.rsqrt(jnp.mean(wide**2, -1, keepdims=True) + 1e-6)


def adamw(w, m, v, g):
    m = 0.9 * m + 0.1 * g
    v = 0.95 * v + 0.05 * g * g
    step = m * lax.rsqrt(v + 1e-8) + 0.1 * w
    return (w - 0.02 * step).astype(BF16), m, v


def silu_parts(gate):
    s = 0.5 * jnp.tanh(0.5 * gate) + 0.5
    y = gate * s
    return y, s + y * (1 - s)


TM = 128
CHUNKS = [(at, min(512, 2816 - at)) for at in range(0, 2816, 512)]
HALVES = [(0, 512), (512, 512)]


def fetch(refs, bufs, sems):
    return [pltpu.make_async_copy(r, b, sems.at[n]) for n, (r, b) in enumerate(zip(refs, bufs))]


def scale_of(h):
    wide = h.astype(F32)
    return wide, lax.rsqrt(jnp.mean(wide * wide, -1, keepdims=True) + 1e-6)


def forth_kernel(x, dy, wg, wu, wd, a0o, g0o, u0o, p0o, h1o, a1o, p1o, dg1o, du1o, wg0, wu0, wd0, wg1, wu1, wd1, sems):
    bufs = (wg0, wu0, wd0, wd1, wg1, wu1)
    copies = fetch([wg.at[0], wu.at[0], wd.at[0], wd.at[1], wg.at[1], wu.at[1]], bufs, sems)
    first = pl.program_id(0) == 0

    def need(*which):
        @pl.when(first)
        def _():
            for n in which:
                copies[n].wait()

    @pl.when(first)
    def _():
        for copy in copies:
            copy.start()

    wide, r = scale_of(x[...])
    a = (wide * r).astype(BF16)
    a0o[...] = a
    need(0, 1)
    for at, size in CHUNKS:
        cols = pl.ds(at, size)
        g = dot(a, wg0[:, cols], (1, 0))
        u = dot(a, wu0[:, cols], (1, 0))
        g0o[:, cols] = g
        u0o[:, cols] = u
        p0o[:, cols] = (silu_parts(g)[0] * u).astype(BF16)
    need(2)
    for at, size in HALVES:
        cols = pl.ds(at, size)
        h1o[:, cols] = x[:, cols] + dot(p0o[...], wd0[:, cols], (1, 0)).astype(BF16)
    wide, r = scale_of(h1o[...])
    a = (wide * r).astype(BF16)
    a1o[...] = a
    need(3, 4, 5)
    d = dy[...]
    for at, size in CHUNKS:
        cols = pl.ds(at, size)
        g = dot(a, wg1[:, cols], (1, 0))
        u = dot(a, wu1[:, cols], (1, 0))
        dp = dot(d, wd1[cols, :], (1, 1)).astype(BF16).astype(F32)
        s, ds = silu_parts(g)
        p1o[:, cols] = (s * u).astype(BF16)
        dg1o[:, cols] = (dp * u * ds).astype(BF16)
        du1o[:, cols] = (dp * s).astype(BF16)


def forth(x, dy, wg, wu, wd):
    tokens, d = x.shape
    ff = wg.shape[2]
    spec = lambda n: pl.BlockSpec((TM, n), lambda i: (i, 0))
    outs = [(d, BF16), (ff, F32), (ff, F32), (ff, BF16), (d, BF16), (d, BF16), (ff, BF16), (ff, BF16), (ff, BF16)]
    return pl.pallas_call(
        forth_kernel,
        name="forth",
        grid=(tokens // TM,),
        in_specs=[spec(d), spec(d)] + [pl.BlockSpec(memory_space=pl.ANY)] * 3,
        out_specs=[spec(n) for n, _ in outs],
        out_shape=[jax.ShapeDtypeStruct((tokens, n), t) for n, t in outs],
        scratch_shapes=[pltpu.VMEM(s, BF16) for s in ((d, ff), (d, ff), (ff, d)) * 2] + [pltpu.SemaphoreType.DMA((6,))],
        compiler_params=pltpu.CompilerParams(vmem_limit_bytes=62 * 2**20, dimension_semantics=("arbitrary",)),
        cost_estimate=pl.CostEstimate(flops=12 * tokens * d * ff, bytes_accessed=180 * 2**20, transcendentals=2 * tokens * ff),
    )(x, dy, wg, wu, wd)


def back_body(step, tick, dg1, du1, dy, h1, g0, u0, wg, wu, wd, dh1o, dg0o, du0o, wg1, wu1, wd0, sems):
    copies = fetch([wg.at[1], wu.at[1], wd.at[0]], (wg1, wu1, wd0), sems)

    @pl.when(step == 0)
    def _():
        for copy in copies:
            copy.start()
        for copy in copies:
            copy.wait()

    tick(0)
    by_gate = dot(dg1[...], wg1[...], (1, 1)).astype(BF16)
    tick(1)
    by_up = dot(du1[...], wu1[...], (1, 1)).astype(BF16)
    da = (by_gate + by_up).astype(F32)
    wide, r = scale_of(h1[...])
    inner = jnp.mean(da * wide, -1, keepdims=True)
    dh1o[...] = dy[...] + (da * r - wide * (r * r * r) * inner).astype(BF16)
    d = dh1o[...]
    for n, (at, size) in enumerate(CHUNKS):
        if n % 3 == 0:
            tick(2 + n // 3)
        cols = pl.ds(at, size)
        dp = dot(d, wd0[cols, :], (1, 1)).astype(BF16).astype(F32)
        s, ds = silu_parts(g0[:, cols])
        dg0o[:, cols] = (dp * u0[:, cols] * ds).astype(BF16)
        du0o[:, cols] = (dp * s).astype(BF16)


def back(dg1, du1, dy, h1, g0, u0, wg, wu, wd, **beside):
    tokens, d = dy.shape
    ff = wg.shape[2]
    tm = 256
    spec = lambda n: pl.BlockSpec((tm, n), lambda i: (i, 0))
    return host(
        "back",
        back_body,
        tokens // tm,
        [spec(n) for n in (ff, ff, d, d, ff, ff)] + [pl.BlockSpec(memory_space=pl.ANY)] * 3,
        [(spec(n), (tokens, n), BF16) for n in (d, ff, ff)],
        (dg1, du1, dy, h1, g0, u0, wg, wu, wd),
        [pltpu.VMEM(s, BF16) for s in ((d, ff), (d, ff), (ff, d))] + [pltpu.SemaphoreType.DMA((3,))],
        flops=6 * tokens * d * ff,
        ticks=4,
        **beside,
    )


def outers(p, d, a, wide, **beside):
    tokens, tile = a.shape[0], 256
    ff, dim = wide[0].shape[1], a.shape[1]
    tiles = ff // tile
    downs = tiles if p is not None else 0
    steps = downs + tiles * len(wide)
    ins, outs, args, scratch = [], [], [], []
    if p is not None:
        ins += [pl.BlockSpec((tokens, tile), lambda i: (0, jnp.minimum(i, tiles - 1))), pl.BlockSpec((tokens, dim), lambda i: (0, 0))]
        outs.append((pl.BlockSpec((tile, dim), lambda i: (jnp.minimum(i, tiles - 1), 0)), (ff, dim), BF16))
        args += [p, d]
    if wide:
        ins.append(pl.BlockSpec((tokens, dim), lambda i: (0, 0)))
        args.append(a)
        scratch.append(pltpu.VMEM((dim, tokens), BF16))

    def column(first):
        return lambda i: (0, jnp.clip(i - first, 0, tiles - 1))

    for n, w in enumerate(wide):
        ins.append(pl.BlockSpec((tokens, tile), column(downs + n * tiles)))
        outs.append((pl.BlockSpec((dim, tile), column(downs + n * tiles)), (dim, ff), BF16))
        args.append(w)

    def work(step, tick, *refs):
        tick(0)
        refs = list(refs)
        if p is not None:
            p_ref, d_ref = refs[:2]
            refs = refs[2:]
        a_ref, w_refs, o_refs, turned = refs[0], refs[1 : 1 + len(wide)], refs[1 + len(wide) : -1], refs[-1]

        if p is not None:

            @pl.when(step < downs)
            def _():
                for at, size in HALVES:
                    o_refs[0][:, pl.ds(at, size)] = dot(p_ref[...], d_ref[:, pl.ds(at, size)], (0, 0)).astype(BF16)

        @pl.when(step == downs)
        def _():
            for at in range(0, tokens, 512):
                turned[:, pl.ds(at, 512)] = a_ref[pl.ds(at, 512), :].T

        for n in range(len(wide)):
            first, w_ref, o_ref = downs + n * tiles, w_refs[n], o_refs[n - len(wide)]

            @pl.when((step >= first) & (step < first + tiles))
            def _():
                o_ref[...] = dot(turned[...], w_ref[...], (1, 0)).astype(BF16)

    return host("outers", work, steps, ins, outs, args, scratch, flops=2 * tokens * tile * dim * steps, **beside)


def outer(a, b, tile=256):
    tokens, m = a.shape
    n = b.shape[1]

    def work(step, tick, a_ref, b_ref, o):
        for at, size in HALVES:
            o[:, pl.ds(at, size)] = dot(a_ref[...], b_ref[:, pl.ds(at, size)], (0, 0)).astype(BF16)

    ins = [pl.BlockSpec((tokens, tile), lambda i: (0, i)), pl.BlockSpec((tokens, n), lambda i: (0, 0))]
    outs = [(pl.BlockSpec((tile, n), lambda i: (i, 0)), (m, n), BF16)]
    return host("outer", work, m // tile, ins, outs, (a, b), flops=2 * tokens * m * n)[0][0]


def body(x, dy, wg, wu, wd, mg, mu, md, vg, vu, vd):
    x, dy = x[0], dy[0]
    i = lax.axis_index(AXES)

    def update(layer, w, m, v, g):
        rows, cols = m.shape[1:]
        mine = lax.dynamic_slice(w, (layer, i * rows, 0), (1, rows, cols))[0].astype(F32)
        return adamw(mine, m[layer], v[layer], g.astype(F32))

    a0, g0, u0, p0, h1, a1, p1, dg1, du1 = forth(x, dy, wg, wu, wd)
    dwd1 = outer(p1, dy)
    (dwg1, dwu1), (sd1,), _ = outers(None, None, a1, [dg1, du1], grads={"d1": dwd1}, collective_id=0)
    (dh1, dg0, du0), (sg1, su1), _ = back(dg1, du1, dy, h1, g0, u0, wg, wu, wd, grads={"g1": dwg1, "u1": dwu1}, collective_id=1)
    nd1, ng1, nu1 = update(1, wd, md, vd, sd1), update(1, wg, mg, vg, sg1), update(1, wu, mu, vu, su1)
    (dwd0, dwg0, dwu0), _, (fd1, fg1, fu1) = outers(p0, dh1, a0, [dg0, du0], blocks={"d": nd1[0], "g": ng1[0], "u": nu1[0]}, collective_id=2)
    _, (sd0, sg0, su0), _ = host("ends", None, 1, [], [], (), grads={"d0": dwd0, "g0": dwg0, "u0": dwu0}, collective_id=3)
    nd0, ng0, nu0 = update(0, wd, md, vd, sd0), update(0, wg, mg, vg, sg0), update(0, wu, mu, vu, su0)
    _, _, (fd0, fg0, fu0) = host("last", None, 1, [], [], (), blocks={"d": nd0[0], "g": ng0[0], "u": nu0[0]}, collective_id=4)
    stacked = [jnp.stack(pair) for pair in ((fg0, fg1), (fu0, fu1), (fd0, fd1))]
    for which in (1, 2):
        stacked += [jnp.stack([a[which], b[which]]) for a, b in ((ng0, ng1), (nu0, nu1), (nd0, nd1))]
    return tuple(stacked)


def solution(mesh):
    whole, seq, part = P(None, None, None), P(("rep", "dp"), None, None), P(None, "dp", None)
    outw, outm = P("rep", None, None), P("rep", "dp", None)
    return jax.shard_map(body, mesh=mesh, in_specs=(seq, seq) + (whole,) * 3 + (part,) * 6, out_specs=(outw,) * 3 + (outm,) * 6, check_vma=False)
```
